32 devices in a mesh: zero: 8 (over z, y), tp: 4 (over x, core).
Axes of the slice: x: 2, y: 2, z: 4, core: 2. Of those that a mesh axis runs over, the one named last changes fastest.
Arguments:
- train_gate: bfloat16 [3072, 8192], P('zero', 'tp'), may hold values from -0.109375 to 0.109375
- low_gate: bfloat16 [3072, 16], P('zero'), may hold values from -0.109375 to 0.109375
- high_gate: bfloat16 [16, 8192], P(None, 'tp'), may hold values from -1.5 to 1.5
- train_up: bfloat16 [3072, 8192], P('zero', 'tp'), may hold values from -0.109375 to 0.109375
- low_up: bfloat16 [3072, 16], P('zero'), may hold values from -0.109375 to 0.109375
- high_up: bfloat16 [16, 8192], P(None, 'tp'), may hold values from -1.5 to 1.5
- train_down: bfloat16 [8192, 3072], P('tp', 'zero'), may hold values from -0.0625 to 0.0625
- low_down: bfloat16 [8192, 16], P('tp'), may hold values from -0.0625 to 0.0625
- high_down: bfloat16 [16, 3072], P(None, 'zero'), may hold values from -1.5 to 1.5
- norm_train: float32 [3072], P(('zero', 'tp')), may hold values from 0.25 to 1.75
- norm_step: float32 [3072], P(('zero', 'tp')), may hold values from -0.3 to 0.3
Outputs:
- serve_gate: bfloat16 [8192, 3072], P('tp')
- serve_up: bfloat16 [8192, 3072], P('tp')
- serve_down: bfloat16 [3072, 8192], P(None, 'tp')
- serve_norm: bfloat16 [3072], replicated
The draws below stay inside these ranges and needn't reach their ends.
All inputs are finite; a program needn't handle non-finite values.
Results may differ from the reference program's by a relative error of at most 0.001.
Values may be sent and summed in bfloat16 or wider, within the bound.
A program may use at most 128 MiB of HBM per device.

```python
import jax
import jax.numpy as jnp

D_MODEL = 3072
D_INNER = 8192
RANK = 16


def block_levels(stream_key, dims, cuts, low, top_value):
    level, own = 1.0, jax.random.fold_in(stream_key, 6)
    for position, parts in cuts:
        draws = jnp.exp(jax.random.uniform(jax.random.fold_in(own, position), (parts,), jnp.float32, low / len(cuts), top_value / len(cuts)))
        level = level * jnp.repeat(draws, dims[position] // parts).reshape([-1 if axis == position else 1 for axis in range(len(dims))])
    return level


def normal_values(own_key, extent, deviation, most, shards=(), dtype=jnp.bfloat16):
    loudness = block_levels(own_key, extent, shards, -0.22, 0.18) if shards else 1.0
    values = jax.random.normal(own_key, extent, jnp.float32) * deviation * loudness
    return jnp.minimum(jnp.maximum(values, -most), most).astype(dtype)


def setup_inputs(seed: int = 0) -> dict:
    splits = jax.random.split(jax.random.key(seed), 12)
    return {
        "train_gate": normal_values(splits[0], (D_MODEL, D_INNER), D_MODEL ** -0.5, 0.109375, ((0, 8), (1, 4))),
        "low_gate": normal_values(splits[1], (D_MODEL, RANK), D_MODEL ** -0.5, 0.109375, ((0, 8),)),
        "high_gate": normal_values(splits[2], (RANK, D_INNER), RANK ** -0.5, 1.5, ((1, 4),)),
        "train_up": normal_values(splits[3], (D_MODEL, D_INNER), D_MODEL ** -0.5, 0.109375, ((0, 8), (1, 4))),
        "low_up": normal_values(splits[4], (D_MODEL, RANK), D_MODEL ** -0.5, 0.109375, ((0, 8),)),
        "high_up": normal_values(splits[5], (RANK, D_INNER), RANK ** -0.5, 1.5, ((1, 4),)),
        "train_down": normal_values(splits[6], (D_INNER, D_MODEL), D_INNER ** -0.5, 0.0625, ((0, 4), (1, 8))),
        "low_down": normal_values(splits[7], (D_INNER, RANK), D_INNER ** -0.5, 0.0625, ((0, 4),)),
        "high_down": normal_values(splits[8], (RANK, D_MODEL), RANK ** -0.5, 1.5, ((1, 8),)),
        "norm_train": jnp.clip(1.0 + 0.15 * jax.random.normal(splits[9], (D_MODEL,), jnp.float32), 0.25, 1.75),
        "norm_step": jnp.clip(jax.random.uniform(splits[10], (D_MODEL,), jnp.float32, -0.3, 0.3) * block_levels(splits[10], (D_MODEL,), ((0, 32),), -0.4, 0.0), -0.3, 0.3),
    }


mix_rate = 0.5


def reference(train_gate, low_gate, high_gate, train_up, low_up, high_up, train_down, low_down, high_down, norm_train, norm_step):
    fresh_gate = train_gate.astype(jnp.float32) + mix_rate * jnp.dot(low_gate, high_gate, preferred_element_type=jnp.float32)
    fresh_up = train_up.astype(jnp.float32) + mix_rate * jnp.dot(low_up, high_up, preferred_element_type=jnp.float32)
    fresh_down = train_down.astype(jnp.float32) + mix_rate * jnp.dot(low_down, high_down, preferred_element_type=jnp.float32)
    serve_gate = fresh_gate.T.astype(jnp.bfloat16)
    serve_up = fresh_up.T.astype(jnp.bfloat16)
    serve_down = fresh_down.T.astype(jnp.bfloat16)
    serve_norm = (norm_train + norm_step).astype(jnp.bfloat16)
    return serve_gate, serve_up, serve_down, serve_norm
```

```python
import functools

import jax
import jax.numpy as jnp
from jax import lax
from jax.experimental import pallas as pl
from jax.experimental.pallas import tpu as pltpu
from jax.sharding import PartitionSpec as P

mix_rate = 0.5
CUTS = 8
PIECES = 3 * CUTS
CROSS = PIECES // 6
STAY = PIECES - CROSS
LINE = PIECES + CROSS
DEPTH = 4
LAG = 4
MESH = pl.DeviceIdType.MESH


def fresh(train, low, high):
    return train.astype(jnp.float32) + mix_rate * jnp.dot(
        low, high, preferred_element_type=jnp.float32
    )


def piece_of(j):
    return jnp.where(
        j < CUTS,
        j,
        jnp.where(j < STAY, j + CROSS, jnp.where(j < PIECES, j - STAY + CUTS, j - PIECES + CUTS)),
    )


def gather_kernel(
    Z, n, m,
    tg, lg, hg, tu, lu, hu, td, ld, hd, nv,
    og, ou, od, nb,
    us, ur, ds, dr, ys, yr, ns, nr, wg, wu, wd, keep,
):
    i, tp = lax.axis_index("zero"), lax.axis_index("tp")
    z, y = i // 2, i % 2
    me = i * m + tp
    depth, width = tg.shape
    cut = width // CUTS

    barrier = pltpu.get_barrier_semaphore()

    def greet(k, _):
        other = lax.rem(me + k, n * m)
        pl.semaphore_signal(
            barrier, inc=1, device_id={"zero": other // m, "tp": lax.rem(other, m)}, device_id_type=MESH
        )
        return 0

    lax.fori_loop(1, n * m, greet, 0)

    def rows_of(source):
        return pl.ds(pl.multiple_of(source * depth, 128), depth)

    def region(which, source, r):
        part = pl.ds(pl.multiple_of(r * cut, cut), cut)
        if which == 2:
            return od.at[rows_of(source), part]
        return (og, ou)[which].at[part, rows_of(source)]

    def own(which, r):
        part = pl.ds(pl.multiple_of(r * cut, cut), cut)
        return wd.at[:, part] if which == 2 else (wg, wu)[which].at[part, :]

    def compute(which, r):
        part = pl.ds(pl.multiple_of(r * cut, cut), cut)
        if which == 2:
            value = fresh(td[part, :], ld[part, :], hd[...])
        else:
            train, low, high = ((tg, lg, hg), (tu, lu, hu))[which]
            value = fresh(train[:, part], low[...], high[:, part])
        own(which, r)[...] = value.T.astype(jnp.bfloat16)

    def compute_range(which, first, last):
        def step(r, _):
            compute(which, r)
            return 0

        lax.fori_loop(first, last, step, 0)

    def start(piece, source, dest, send, recv):
        r = lax.rem(piece, CUTS)

        def go(src, dst):
            pltpu.make_async_remote_copy(
                src, dst, send, recv, device_id={"zero": dest}, device_id_type=MESH
            ).start()

        for which in range(3):
            @pl.when((piece // CUTS == which) & (source == i))
            def _():
                go(own(which, r), region(which, source, r))

            @pl.when((piece // CUTS == which) & (source != i))
            def _():
                go(region(which, source, r), region(which, source, r))

    def waiter(send, recv):
        ref = region(0, 0, 0)
        return pltpu.make_async_remote_copy(
            ref, ref, send, recv, device_id={"zero": i}, device_id_type=MESH
        )

    n_up = jnp.where(z < Z - 1, LINE * (z + 1), 0)
    n_down = jnp.where(z > 0, LINE * (Z - z), 0)
    n_up_in = LINE * z
    n_down_in = LINE * (Z - 1 - z)
    n_side = PIECES + STAY * (Z - 1)
    low_side = jnp.minimum(z, Z - 1 - z)

    def start_line(q, sign, send, recv):
        k, j = q // LINE, lax.rem(q, LINE)
        row = jnp.where(j < PIECES, y, 1 - y)
        start(piece_of(j), (z - sign * k) * 2 + row, (z + sign) * 2 + y, send.at[lax.rem(q, DEPTH)], recv.at[q])

    def start_up(q):
        @pl.when(q < n_up)
        def _():
            start_line(q, 1, us, ur)

    def start_down(q):
        @pl.when(q < n_down)
        def _():
            start_line(q, -1, ds, dr)

    def start_side(q):
        @pl.when(q < n_side)
        def _():
            later = jnp.maximum(q - PIECES, 0)
            b, j = later // STAY, lax.rem(later, STAY)
            paired = b < 2 * low_side
            k = jnp.where(paired, b // 2 + 1, b - low_side + 1)
            back = jnp.where(paired, lax.rem(b, 2) == 0, z > Z - 1 - z)
            source = jnp.where(q < PIECES, z, jnp.where(back, z - k, z + k))
            piece = jnp.where(q < PIECES, q, piece_of(j))
            start(piece, source * 2 + y, z * 2 + 1 - y, ys.at[lax.rem(q, DEPTH)], yr.at[q])

    nb[me] = nv[...]
    compute_range(0, 0, DEPTH + 1)
    pl.semaphore_wait(barrier, n * m - 1)

    def first(q, _):
        start_up(q)
        start_down(q)
        start_side(q)
        return 0

    lax.fori_loop(0, DEPTH, first, 0)
    compute_range(0, DEPTH + 1, CUTS)
    compute_range(1, 0, CUTS)
    compute_range(2, 0, CUTS)
    kept = [
        pltpu.make_async_copy(src, dst, keep.at[which])
        for which, (src, dst) in enumerate((
            (wg, og.at[:, rows_of(i)]), (wu, ou.at[:, rows_of(i)]), (wd, od.at[rows_of(i), :]),
        ))
    ]
    for copy in kept:
        copy.start()

    def norm_copy(k):
        other = lax.rem(me + k, n * m)
        return pltpu.make_async_remote_copy(
            nb.at[me], nb.at[me], ns.at[k], nr.at[me],
            device_id={"zero": other // m, "tp": lax.rem(other, m)}, device_id_type=MESH,
        )

    def norm_send(k, _):
        norm_copy(k).start()
        return 0

    lax.fori_loop(1, n * m, norm_send, 0)

    def step(t, _):
        p = t - LAG
        at = jnp.maximum(p, 0)

        @pl.when((p >= 0) & (p < n_up_in))
        def _():
            waiter(us.at[0], ur.at[at]).wait_recv()

        @pl.when((p >= 0) & (p < n_down_in))
        def _():
            waiter(ds.at[0], dr.at[at]).wait_recv()

        @pl.when((p >= 0) & (p < n_side))
        def _():
            waiter(ys.at[0], yr.at[at]).wait_recv()

        slot = lax.rem(t, DEPTH)

        @pl.when(t < n_up)
        def _():
            waiter(us.at[slot], ur.at[0]).wait_send()

        start_up(t + DEPTH)

        @pl.when(t < n_down)
        def _():
            waiter(ds.at[slot], dr.at[0]).wait_send()

        start_down(t + DEPTH)

        @pl.when(t < n_side)
        def _():
            waiter(ys.at[slot], yr.at[0]).wait_send()

        start_side(t + DEPTH)
        return 0

    steps = max(LINE * (Z - 1), PIECES + STAY * (Z - 1)) + LAG
    lax.fori_loop(0, steps, step, 0)

    def norm_wait(k, _):
        other = lax.rem(me + k, n * m)
        norm_copy(k).wait_send()
        pltpu.make_async_remote_copy(
            nb.at[other], nb.at[other], ns.at[k], nr.at[other],
            device_id={"zero": i}, device_id_type=MESH,
        ).wait_recv()
        return 0

    lax.fori_loop(1, n * m, norm_wait, 0)
    for copy in kept:
        copy.wait()


def fast(
    n, m,
    train_gate, low_gate, high_gate,
    train_up, low_up, high_up,
    train_down, low_down, high_down,
    norm_train, norm_step,
):
    depth, width = train_gate.shape
    Z = n // 2
    gain = norm_train + norm_step
    share = gain.shape[0]
    lanes = -(-share // 128) * 128
    nv = jnp.broadcast_to(jnp.pad(gain, (0, lanes - share))[None], (8, lanes))
    n_line, n_side = LINE * (Z - 1), PIECES + STAY * (Z - 1)
    dma = pltpu.SemaphoreType.DMA
    outs = pl.pallas_call(
        functools.partial(gather_kernel, Z, n, m),
        out_shape=(
            jax.ShapeDtypeStruct((width, n * depth), jnp.bfloat16),
            jax.ShapeDtypeStruct((width, n * depth), jnp.bfloat16),
            jax.ShapeDtypeStruct((n * depth, width), jnp.bfloat16),
            jax.ShapeDtypeStruct((n * m, 8, lanes), jnp.float32),
        ),
        in_specs=[pl.BlockSpec(memory_space=pltpu.VMEM)] * 10,
        out_specs=(pl.BlockSpec(memory_space=pl.ANY),) * 3 + (pl.BlockSpec(memory_space=pltpu.VMEM),),
        scratch_shapes=[
            dma((DEPTH,)), dma((n_line,)),
            dma((DEPTH,)), dma((n_line,)),
            dma((DEPTH,)), dma((n_side,)),
            dma((n * m,)), dma((n * m,)),
            pltpu.VMEM((width, depth), jnp.bfloat16),
            pltpu.VMEM((width, depth), jnp.bfloat16),
            pltpu.VMEM((depth, width), jnp.bfloat16),
            dma((3,)),
        ],
        compiler_params=pltpu.CompilerParams(
            collective_id=0, has_side_effects=True
        ),
    )(
        train_gate, low_gate, high_gate,
        train_up, low_up, high_up,
        train_down, low_down, high_down,
        nv,
    )
    serve_gate, serve_up, serve_down, norms = outs
    serve_norm = norms[:, 0, :share].reshape(-1).astype(jnp.bfloat16)
    return serve_gate, serve_up, serve_down, serve_norm


def plain(
    train_gate, low_gate, high_gate,
    train_up, low_up, high_up,
    train_down, low_down, high_down,
    norm_train, norm_step,
):
    serve_gate = lax.all_gather(
        fresh(train_gate, low_gate, high_gate).astype(jnp.bfloat16), "zero", axis=0, tiled=True
    ).T
    serve_up = lax.all_gather(
        fresh(train_up, low_up, high_up).astype(jnp.bfloat16), "zero", axis=0, tiled=True
    ).T
    serve_down = lax.all_gather(
        fresh(train_down, low_down, high_down).astype(jnp.bfloat16), "zero", axis=1, tiled=True
    ).T
    serve_norm = lax.all_gather(
        (norm_train + norm_step).astype(jnp.bfloat16), ("zero", "tp"), axis=0, tiled=True
    )
    return serve_gate, serve_up, serve_down, serve_norm


def per_device(n, m, *args):
    depth, width = args[0].shape
    fits = (
        n % 2 == 0
        and 2 <= n // 2 <= 4
        and depth % 128 == 0
        and width % (CUTS * 128) == 0
        and args[6].shape == (width, depth)
        and 6 * n * depth * width <= 40 * 1024 * 1024
    )
    return fast(n, m, *args) if fits else plain(*args)


def solution(mesh):
    return jax.shard_map(
        functools.partial(per_device, mesh.shape["zero"], mesh.shape["tp"]),
        mesh=mesh,
        in_specs=(
            P("zero", "tp"),
            P("zero", None),
            P(None, "tp"),
            P("zero", "tp"),
            P("zero", None),
            P(None, "tp"),
            P("tp", "zero"),
            P("tp", None),
            P(None, "zero"),
            P(("zero", "tp")),
            P(("zero", "tp")),
        ),
        out_specs=(P("tp", None), P("tp", None), P(None, "tp"), P()),
        check_vma=False,
    )
```

```python
import functools

import jax
import jax.numpy as jnp
from jax import lax
from jax.experimental import pallas as pl
from jax.experimental.pallas import tpu as pltpu
from jax.sharding import PartitionSpec as P

mix_rate = 0.5
CUTS = 8
PIECES = 3 * CUTS
CROSS = PIECES // 6
STAY = PIECES - CROSS
LINE = PIECES + CROSS
DEPTH = 4
AHEAD = 2
LAG = 4
MESH = pl.DeviceIdType.MESH


def fresh(train, low_t, high):
    return train.astype(jnp.float32) + mix_rate * lax.dot_general(
        low_t, high, (((0,), (0,)), ((), ())), preferred_element_type=jnp.float32
    )


def piece_of(j):
    return jnp.where(
        j < CUTS,
        j,
        jnp.where(j < STAY, j + CROSS, jnp.where(j < PIECES, j - STAY + CUTS, j - PIECES + CUTS)),
    )


def gather_kernel(
    Z, n, m,
    tg, lg, hg, tu, lu, hu, td, ld, hd, nt, nd,
    held, nb,
    us, ur, ds, dr, ys, yr, ns, nr, vu, vd, fetch,
):
    i, tp = lax.axis_index("zero"), lax.axis_index("tp")
    z, y = i // 2, i % 2
    me = i * m + tp
    depth, width = tg.shape
    cut = width // CUTS

    fetch_up = pltpu.make_async_copy(tu, vu, fetch.at[0])
    fetch_down = pltpu.make_async_copy(td, vd, fetch.at[1])
    fetch_up.start()
    fetch_down.start()
    barrier = pltpu.get_barrier_semaphore()

    def greet(k, _):
        other = lax.rem(me + k, n * m)
        pl.semaphore_signal(
            barrier, inc=1, device_id={"zero": other // m, "tp": lax.rem(other, m)}, device_id_type=MESH
        )
        return 0

    lax.fori_loop(1, n * m, greet, 0)

    tiles = depth // 128

    def region(which, source, r):
        return held.at[which, pl.ds(source * tiles, tiles), pl.ds(pl.multiple_of(r * cut, cut), cut), :]

    def compute(which, r):
        part = pl.ds(pl.multiple_of(r * cut, cut), cut)
        if which == 2:
            value = fresh(vd[part, :], ld[:, part], hd[...])
        else:
            train, low, high = ((tg, lg, hg), (vu, lu, hu))[which]
            value = fresh(train[:, part], low[...], high[:, part])
        served = value.T.astype(jnp.bfloat16)
        for a in range(tiles):
            if which == 2:
                for b in range(cut // 128):
                    held[2, i * tiles + a, pl.ds(pl.multiple_of(r * cut + b * 128, 128), 128), :] = (
                        served[a * 128 : (a + 1) * 128, b * 128 : (b + 1) * 128]
                    )
            else:
                held[which, i * tiles + a, part, :] = served[:, a * 128 : (a + 1) * 128]

    def compute_range(which, first, last):
        def step(r, _):
            compute(which, r)
            return 0

        lax.fori_loop(first, last, step, 0)

    def start(piece, source, dest, send, recv):
        ref = region(piece // CUTS, source, lax.rem(piece, CUTS))
        pltpu.make_async_remote_copy(
            ref, ref, send, recv, device_id={"zero": dest}, device_id_type=MESH
        ).start()

    def waiter(send, recv):
        ref = region(0, 0, 0)
        return pltpu.make_async_remote_copy(
            ref, ref, send, recv, device_id={"zero": i}, device_id_type=MESH
        )

    n_up = jnp.where(z < Z - 1, LINE * (z + 1), 0)
    n_down = jnp.where(z > 0, LINE * (Z - z), 0)
    n_up_in = LINE * z
    n_down_in = LINE * (Z - 1 - z)
    n_side = PIECES + STAY * (Z - 1)
    low_side = jnp.minimum(z, Z - 1 - z)

    def start_line(q, sign, send, recv):
        k, j = q // LINE, lax.rem(q, LINE)
        row = jnp.where(j < PIECES, y, 1 - y)
        start(piece_of(j), (z - sign * k) * 2 + row, (z + sign) * 2 + y, send.at[lax.rem(q, DEPTH)], recv.at[q])

    def start_up(q):
        @pl.when(q < n_up)
        def _():
            start_line(q, 1, us, ur)

    def start_down(q):
        @pl.when(q < n_down)
        def _():
            start_line(q, -1, ds, dr)

    def start_side(q):
        @pl.when(q < n_side)
        def _():
            later = jnp.maximum(q - PIECES, 0)
            b, j = later // STAY, lax.rem(later, STAY)
            paired = b < 2 * low_side
            k = jnp.where(paired, b // 2 + 1, b - low_side + 1)
            back = jnp.where(paired, lax.rem(b, 2) == 0, z > Z - 1 - z)
            source = jnp.where(q < PIECES, z, jnp.where(back, z - k, z + k))
            piece = jnp.where(q < PIECES, q, piece_of(j))
            start(piece, source * 2 + y, z * 2 + 1 - y, ys.at[lax.rem(q, DEPTH)], yr.at[q])

    nb[me] = jnp.zeros(nb.shape[1:], nb.dtype)
    nb[me, 0:1, : nt.shape[1]] = nt[...] + nd[...]
    compute_range(0, 0, AHEAD)
    pl.semaphore_wait(barrier, n * m - 1)

    def first(q, _):
        start_up(q)
        start_down(q)
        start_side(q)
        compute(0, q + AHEAD)
        return 0

    lax.fori_loop(0, DEPTH, first, 0)
    compute_range(0, DEPTH + AHEAD, CUTS)
    fetch_up.wait()
    compute_range(1, 0, CUTS)
    fetch_down.wait()
    compute_range(2, 0, CUTS)
    def norm_copy(k):
        other = lax.rem(me + k, n * m)
        return pltpu.make_async_remote_copy(
            nb.at[me], nb.at[me], ns.at[k], nr.at[me],
            device_id={"zero": other // m, "tp": lax.rem(other, m)}, device_id_type=MESH,
        )

    def norm_send(k, _):
        norm_copy(k).start()
        return 0

    lax.fori_loop(1, n * m, norm_send, 0)

    def step(t, _):
        p = t - LAG
        at = jnp.maximum(p, 0)

        @pl.when((p >= 0) & (p < n_up_in))
        def _():
            waiter(us.at[0], ur.at[at]).wait_recv()

        @pl.when((p >= 0) & (p < n_down_in))
        def _():
            waiter(ds.at[0], dr.at[at]).wait_recv()

        @pl.when((p >= 0) & (p < n_side))
        def _():
            waiter(ys.at[0], yr.at[at]).wait_recv()

        slot = lax.rem(t, DEPTH)

        @pl.when(t < n_up)
        def _():
            waiter(us.at[slot], ur.at[0]).wait_send()

        start_up(t + DEPTH)

        @pl.when(t < n_down)
        def _():
            waiter(ds.at[slot], dr.at[0]).wait_send()

        start_down(t + DEPTH)

        @pl.when(t < n_side)
        def _():
            waiter(ys.at[slot], yr.at[0]).wait_send()

        start_side(t + DEPTH)
        return 0

    steps = max(LINE * (Z - 1), PIECES + STAY * (Z - 1)) + LAG
    lax.fori_loop(0, steps, step, 0)

    def norm_wait(k, _):
        other = lax.rem(me + k, n * m)
        norm_copy(k).wait_send()
        pltpu.make_async_remote_copy(
            nb.at[other], nb.at[other], ns.at[k], nr.at[other],
            device_id={"zero": i}, device_id_type=MESH,
        ).wait_recv()
        return 0

    lax.fori_loop(1, n * m, norm_wait, 0)


def settle_kernel(held, og, ou, od, done):
    _, groups, width, _ = held.shape

    def group(c, _):
        span = pl.ds(pl.multiple_of(c * 128, 128), 128)
        pltpu.make_async_copy(held.at[0, c], og.at[:, span], done.at[0]).start()
        pltpu.make_async_copy(held.at[1, c], ou.at[:, span], done.at[1]).start()
        for d in range(width // 128):
            part = pl.ds(d * 128, 128)
            pltpu.make_async_copy(held.at[2, c, part, :], od.at[span, part], done.at[2]).start()
        return 0

    lax.fori_loop(0, groups, group, 0)
    for k, ref in enumerate((og, ou, od)):
        pltpu.make_async_copy(ref, ref, done.at[k]).wait()


def fast(
    n, m,
    train_gate, low_gate, high_gate,
    train_up, low_up, high_up,
    train_down, low_down, high_down,
    norm_train, norm_step,
):
    depth, width = train_gate.shape
    Z = n // 2
    share = norm_train.shape[0]
    lanes = -(-share // 128) * 128
    n_line, n_side = LINE * (Z - 1), PIECES + STAY * (Z - 1)
    dma = pltpu.SemaphoreType.DMA
    held, norms = pl.pallas_call(
        functools.partial(gather_kernel, Z, n, m),
        out_shape=(
            pltpu.VMEM((3, n * depth // 128, width, 128), jnp.bfloat16),
            jax.ShapeDtypeStruct((n * m, 8, lanes), jnp.float32),
        ),
        in_specs=[
            pl.BlockSpec(memory_space=pl.ANY if k in (3, 6) else pltpu.VMEM) for k in range(11)
        ],
        out_specs=(pl.BlockSpec(memory_space=pltpu.VMEM),) * 2,
        scratch_shapes=[
            dma((DEPTH,)), dma((n_line,)),
            dma((DEPTH,)), dma((n_line,)),
            dma((DEPTH,)), dma((n_side,)),
            dma((n * m,)), dma((n * m,)),
            pltpu.VMEM(train_up.shape, jnp.bfloat16),
            pltpu.VMEM(train_down.shape, jnp.bfloat16),
            dma((2,)),
        ],
        compiler_params=pltpu.CompilerParams(
            collective_id=0, has_side_effects=True, vmem_limit_bytes=27 * 1024 * 1024
        ),
    )(
        train_gate, low_gate.T, high_gate,
        train_up, low_up.T, high_up,
        train_down, low_down.T, high_down,
        norm_train[None], norm_step[None],
    )
    serve_gate, serve_up, serve_down = pl.pallas_call(
        settle_kernel,
        out_shape=(
            jax.ShapeDtypeStruct((width, n * depth), jnp.bfloat16),
            jax.ShapeDtypeStruct((width, n * depth), jnp.bfloat16),
            jax.ShapeDtypeStruct((n * depth, width), jnp.bfloat16),
        ),
        in_specs=[pl.BlockSpec(memory_space=pltpu.VMEM)],
        out_specs=(pl.BlockSpec(memory_space=pl.ANY),) * 3,
        scratch_shapes=[dma((3,))],
        compiler_params=pltpu.CompilerParams(vmem_limit_bytes=1024 * 1024),
    )(pltpu.with_memory_space_constraint(held, pltpu.VMEM))
    serve_norm = norms[:, 0, :share].reshape(-1).astype(jnp.bfloat16)
    return serve_gate, serve_up, serve_down, serve_norm


def plain(
    train_gate, low_gate, high_gate,
    train_up, low_up, high_up,
    train_down, low_down, high_down,
    norm_train, norm_step,
):
    serve_gate = lax.all_gather(
        fresh(train_gate, low_gate.T, high_gate).astype(jnp.bfloat16), "zero", axis=0, tiled=True
    ).T
    serve_up = lax.all_gather(
        fresh(train_up, low_up.T, high_up).astype(jnp.bfloat16), "zero", axis=0, tiled=True
    ).T
    serve_down = lax.all_gather(
        fresh(train_down, low_down.T, high_down).astype(jnp.bfloat16), "zero", axis=1, tiled=True
    ).T
    serve_norm = lax.all_gather(
        (norm_train + norm_step).astype(jnp.bfloat16), ("zero", "tp"), axis=0, tiled=True
    )
    return serve_gate, serve_up, serve_down, serve_norm


def per_device(n, m, *args):
    depth, width = args[0].shape
    fits = (
        n % 2 == 0
        and 2 <= n // 2 <= 4
        and depth % 128 == 0
        and width % (CUTS * 128) == 0
        and args[6].shape == (width, depth)
        and 6 * n * depth * width <= 40 * 1024 * 1024
    )
    return fast(n, m, *args) if fits else plain(*args)


def solution(mesh):
    return jax.shard_map(
        functools.partial(per_device, mesh.shape["zero"], mesh.shape["tp"]),
        mesh=mesh,
        in_specs=(
            P("zero", "tp"),
            P("zero", None),
            P(None, "tp"),
            P("zero", "tp"),
            P("zero", None),
            P(None, "tp"),
            P("tp", "zero"),
            P("tp", None),
            P(None, "zero"),
            P(("zero", "tp")),
            P(("zero", "tp")),
        ),
        out_specs=(P("tp", None), P("tp", None), P(None, "tp"), P()),
        check_vma=False,
    )
```

```python
import functools

import jax
import jax.numpy as jnp
from jax import lax
from jax.experimental import pallas as pl
from jax.experimental.pallas import tpu as pltpu
from jax.sharding import PartitionSpec as P

mix_rate = 0.5
CUTS = 16
PIECES = 3 * CUTS
CROSS = PIECES // 6
STAY = PIECES - CROSS
LINE = PIECES + CROSS
DEPTH = 6
AHEAD = 2
LAG = 6
MESH = pl.DeviceIdType.MESH


def fresh(train, low_t, high):
    return train.astype(jnp.float32) + mix_rate * lax.dot_general(
        low_t, high, (((0,), (0,)), ((), ())), preferred_element_type=jnp.float32
    )


def piece_of(j):
    return jnp.where(
        j < CUTS,
        j,
        jnp.where(j < STAY, j + CROSS, jnp.where(j < PIECES, j - STAY + CUTS, j - PIECES + CUTS)),
    )


def gather_kernel(
    Z, n, m,
    tg, lg, hg, tu, lu, hu, td, ld, hd, nt, nd,
    held, nb,
    us, ur, ds, dr, ys, yr, ns, nr, vu, vd, fetch,
):
    i, tp = lax.axis_index("zero"), lax.axis_index("tp")
    z, y = i // 2, i % 2
    me = i * m + tp
    depth, width = tg.shape
    cut = width // CUTS

    fetch_up = pltpu.make_async_copy(tu, vu, fetch.at[0])
    fetch_down = pltpu.make_async_copy(td, vd, fetch.at[1])
    fetch_up.start()
    fetch_down.start()
    barrier = pltpu.get_barrier_semaphore()

    def greet(k, _):
        other = lax.rem(me + k, n * m)
        pl.semaphore_signal(
            barrier, inc=1, device_id={"zero": other // m, "tp": lax.rem(other, m)}, device_id_type=MESH
        )
        return 0

    lax.fori_loop(1, n * m, greet, 0)

    tiles = depth // 128

    def region(which, source, r):
        return held.at[which, pl.ds(source * tiles, tiles), pl.ds(pl.multiple_of(r * cut, cut), cut), :]

    def compute(which, r):
        part = pl.ds(pl.multiple_of(r * cut, cut), cut)
        if which == 2:
            value = fresh(vd[part, :], ld[:, part], hd[...])
        else:
            train, low, high = ((tg, lg, hg), (vu, lu, hu))[which]
            value = fresh(train[:, part], low[...], high[:, part])
        served = value.T.astype(jnp.bfloat16)
        for a in range(tiles):
            if which == 2:
                for b in range(cut // 128):
                    held[2, i * tiles + a, pl.ds(pl.multiple_of(r * cut + b * 128, 128), 128), :] = (
                        served[a * 128 : (a + 1) * 128, b * 128 : (b + 1) * 128]
                    )
            else:
                held[which, i * tiles + a, part, :] = served[:, a * 128 : (a + 1) * 128]

    def compute_range(which, first, last):
        def step(r, _):
            compute(which, r)
            return 0

        lax.fori_loop(first, last, step, 0)

    def start(piece, source, dest, send, recv):
        ref = region(piece // CUTS, source, lax.rem(piece, CUTS))
        pltpu.make_async_remote_copy(
            ref, ref, send, recv, device_id={"zero": dest}, device_id_type=MESH
        ).start()

    def waiter(send, recv):
        ref = region(0, 0, 0)
        return pltpu.make_async_remote_copy(
            ref, ref, send, recv, device_id={"zero": i}, device_id_type=MESH
        )

    n_up = jnp.where(z < Z - 1, LINE * (z + 1), 0)
    n_down = jnp.where(z > 0, LINE * (Z - z), 0)
    n_up_in = LINE * z
    n_down_in = LINE * (Z - 1 - z)
    n_side = PIECES + STAY * (Z - 1)
    low_side = jnp.minimum(z, Z - 1 - z)

    def start_line(q, sign, send, recv):
        k, j = q // LINE, lax.rem(q, LINE)
        row = jnp.where(j < PIECES, y, 1 - y)
        start(piece_of(j), (z - sign * k) * 2 + row, (z + sign) * 2 + y, send.at[lax.rem(q, DEPTH)], recv.at[q])

    def start_up(q):
        @pl.when(q < n_up)
        def _():
            start_line(q, 1, us, ur)

    def start_down(q):
        @pl.when(q < n_down)
        def _():
            start_line(q, -1, ds, dr)

    def start_side(q):
        @pl.when(q < n_side)
        def _():
            later = jnp.maximum(q - PIECES, 0)
            b, j = later // STAY, lax.rem(later, STAY)
            paired = b < 2 * low_side
            k = jnp.where(paired, b // 2 + 1, b - low_side + 1)
            back = jnp.where(paired, lax.rem(b, 2) == 0, z > Z - 1 - z)
            source = jnp.where(q < PIECES, z, jnp.where(back, z - k, z + k))
            piece = jnp.where(q < PIECES, q, piece_of(j))
            start(piece, source * 2 + y, z * 2 + 1 - y, ys.at[lax.rem(q, DEPTH)], yr.at[q])

    nb[me] = jnp.zeros(nb.shape[1:], nb.dtype)
    nb[me, 0:1, : nt.shape[1]] = nt[...] + nd[...]
    compute_range(0, 0, AHEAD)
    pl.semaphore_wait(barrier, n * m - 1)

    def first(q, _):
        start_up(q)
        start_down(q)
        start_side(q)
        compute(0, q + AHEAD)
        return 0

    lax.fori_loop(0, DEPTH, first, 0)
    compute_range(0, DEPTH + AHEAD, CUTS)
    fetch_up.wait()
    compute_range(1, 0, CUTS)
    fetch_down.wait()
    compute_range(2, 0, CUTS)
    def norm_copy(k):
        other = lax.rem(me + k, n * m)
        return pltpu.make_async_remote_copy(
            nb.at[me], nb.at[me], ns.at[k], nr.at[me],
            device_id={"zero": other // m, "tp": lax.rem(other, m)}, device_id_type=MESH,
        )

    def norm_send(k, _):
        norm_copy(k).start()
        return 0

    lax.fori_loop(1, n * m, norm_send, 0)

    def step(t, _):
        p = t - LAG
        at = jnp.maximum(p, 0)

        @pl.when((p >= 0) & (p < n_up_in))
        def _():
            waiter(us.at[0], ur.at[at]).wait_recv()

        @pl.when((p >= 0) & (p < n_down_in))
        def _():
            waiter(ds.at[0], dr.at[at]).wait_recv()

        @pl.when((p >= 0) & (p < n_side))
        def _():
            waiter(ys.at[0], yr.at[at]).wait_recv()

        slot = lax.rem(t, DEPTH)

        @pl.when(t < n_up)
        def _():
            waiter(us.at[slot], ur.at[0]).wait_send()

        start_up(t + DEPTH)

        @pl.when(t < n_down)
        def _():
            waiter(ds.at[slot], dr.at[0]).wait_send()

        start_down(t + DEPTH)

        @pl.when(t < n_side)
        def _():
            waiter(ys.at[slot], yr.at[0]).wait_send()

        start_side(t + DEPTH)
        return 0

    steps = max(LINE * (Z - 1), PIECES + STAY * (Z - 1)) + LAG
    lax.fori_loop(0, steps, step, 0)

    def norm_wait(k, _):
        other = lax.rem(me + k, n * m)
        norm_copy(k).wait_send()
        pltpu.make_async_remote_copy(
            nb.at[other], nb.at[other], ns.at[k], nr.at[other],
            device_id={"zero": i}, device_id_type=MESH,
        ).wait_recv()
        return 0

    lax.fori_loop(1, n * m, norm_wait, 0)


def settle_kernel(held, og, ou, od, done):
    _, groups, width, _ = held.shape

    def group(c, _):
        span = pl.ds(pl.multiple_of(c * 128, 128), 128)
        pltpu.make_async_copy(held.at[0, c], og.at[:, span], done.at[0]).start()
        pltpu.make_async_copy(held.at[1, c], ou.at[:, span], done.at[1]).start()
        for d in range(width // 128):
            part = pl.ds(d * 128, 128)
            pltpu.make_async_copy(held.at[2, c, part, :], od.at[span, part], done.at[2]).start()
        return 0

    lax.fori_loop(0, groups, group, 0)
    for k, ref in enumerate((og, ou, od)):
        pltpu.make_async_copy(ref, ref, done.at[k]).wait()


def fast(
    n, m,
    train_gate, low_gate, high_gate,
    train_up, low_up, high_up,
    train_down, low_down, high_down,
    norm_train, norm_step,
):
    depth, width = train_gate.shape
    Z = n // 2
    share = norm_train.shape[0]
    lanes = -(-share // 128) * 128
    n_line, n_side = LINE * (Z - 1), PIECES + STAY * (Z - 1)
    dma = pltpu.SemaphoreType.DMA
    held, norms = pl.pallas_call(
        functools.partial(gather_kernel, Z, n, m),
        out_shape=(
            pltpu.VMEM((3, n * depth // 128, width, 128), jnp.bfloat16),
            jax.ShapeDtypeStruct((n * m, 8, lanes), jnp.float32),
        ),
        in_specs=[
            pl.BlockSpec(memory_space=pl.ANY if k in (3, 6) else pltpu.VMEM) for k in range(11)
        ],
        out_specs=(pl.BlockSpec(memory_space=pltpu.VMEM),) * 2,
        scratch_shapes=[
            dma((DEPTH,)), dma((n_line,)),
            dma((DEPTH,)), dma((n_line,)),
            dma((DEPTH,)), dma((n_side,)),
            dma((n * m,)), dma((n * m,)),
            pltpu.VMEM(train_up.shape, jnp.bfloat16),
            pltpu.VMEM(train_down.shape, jnp.bfloat16),
            dma((2,)),
        ],
        compiler_params=pltpu.CompilerParams(
            collective_id=0, has_side_effects=True, vmem_limit_bytes=27 * 1024 * 1024
        ),
    )(
        train_gate, low_gate.T, high_gate,
        train_up, low_up.T, high_up,
        train_down, low_down.T, high_down,
        norm_train[None], norm_step[None],
    )
    serve_gate, serve_up, serve_down = pl.pallas_call(
        settle_kernel,
        out_shape=(
            jax.ShapeDtypeStruct((width, n * depth), jnp.bfloat16),
            jax.ShapeDtypeStruct((width, n * depth), jnp.bfloat16),
            jax.ShapeDtypeStruct((n * depth, width), jnp.bfloat16),
        ),
        in_specs=[pl.BlockSpec(memory_space=pltpu.VMEM)],
        out_specs=(pl.BlockSpec(memory_space=pl.ANY),) * 3,
        scratch_shapes=[dma((3,))],
        compiler_params=pltpu.CompilerParams(vmem_limit_bytes=1024 * 1024),
    )(pltpu.with_memory_space_constraint(held, pltpu.VMEM))
    serve_norm = norms[:, 0, :share].reshape(-1).astype(jnp.bfloat16)
    return serve_gate, serve_up, serve_down, serve_norm


def plain(
    train_gate, low_gate, high_gate,
    train_up, low_up, high_up,
    train_down, low_down, high_down,
    norm_train, norm_step,
):
    serve_gate = lax.all_gather(
        fresh(train_gate, low_gate.T, high_gate).astype(jnp.bfloat16), "zero", axis=0, tiled=True
    ).T
    serve_up = lax.all_gather(
        fresh(train_up, low_up.T, high_up).astype(jnp.bfloat16), "zero", axis=0, tiled=True
    ).T
    serve_down = lax.all_gather(
        fresh(train_down, low_down.T, high_down).astype(jnp.bfloat16), "zero", axis=1, tiled=True
    ).T
    serve_norm = lax.all_gather(
        (norm_train + norm_step).astype(jnp.bfloat16), ("zero", "tp"), axis=0, tiled=True
    )
    return serve_gate, serve_up, serve_down, serve_norm


def per_device(n, m, *args):
    depth, width = args[0].shape
    fits = (
        n % 2 == 0
        and 2 <= n // 2 <= 4
        and depth % 128 == 0
        and width % (CUTS * 128) == 0
        and args[6].shape == (width, depth)
        and 6 * n * depth * width <= 40 * 1024 * 1024
    )
    return fast(n, m, *args) if fits else plain(*args)


def solution(mesh):
    return jax.shard_map(
        functools.partial(per_device, mesh.shape["zero"], mesh.shape["tp"]),
        mesh=mesh,
        in_specs=(
            P("zero", "tp"),
            P("zero", None),
            P(None, "tp"),
            P("zero", "tp"),
            P("zero", None),
            P(None, "tp"),
            P("tp", "zero"),
            P("tp", None),
            P(None, "zero"),
            P(("zero", "tp")),
            P(("zero", "tp")),
        ),
        out_specs=(P("tp", None), P("tp", None), P(None, "tp"), P()),
        check_vma=False,
    )
```
